1024 devices in a mesh: ep: 64 (over x, z), tp: 16 (over y, core).
Axes of the slice: x: 4, y: 8, z: 16, core: 2. Of those that a mesh axis runs over, the one named last changes fastest.
Arguments:
- tokens: bfloat16 [8192, 3584], P('ep', 'tp'), may hold values from -6 to 6
- routes: int32 [8192, 8], P('ep'), may hold values from 0 to 63, all different within a row; in each aligned block of 128 rows (0 to 127, 128 to 255, ...) at most 18 rows name the same one
- gate_levels: int32 [8192, 8], P('ep'), may hold values from 1 to 255
- w_gate: bfloat16 [64, 3584, 1024], P('ep', 'tp'), may hold values from -0.09375 to 0.09375
- w_up: bfloat16 [64, 3584, 1024], P('ep', 'tp'), may hold values from -0.09375 to 0.09375
- w_down: bfloat16 [64, 1024, 3584], P('ep', None, 'tp'), may hold values from -0.1875 to 0.1875
Outputs:
- mixed: bfloat16 [8192, 3584], P('ep', 'tp')
The draws below stay inside these ranges and needn't reach their ends.
Inputs may be any that keep to these rules, and one draw needn't show every extreme that they name: `routes`: each row names 8 different experts. Among the 128 tokens of one aligned block no expert is named by more than 18 rows, and in every draw some expert is named by exactly 18 rows of some block.
All inputs are finite; a program needn't handle non-finite values.
Results may differ from the reference program's by a relative error of at most 0.0085.
Values may be sent and summed in bfloat16 or wider, within the bound.
A program may use at most 64 MiB of HBM per device.

```python
import math
import jax
import jax.numpy as jnp
import numpy as np
from jax import lax

D = 3584
FF = 1024
TOP = 8
TOK_EP = 128
EXPERTS = 64
CAP = 18
TOKENS = 8192
N_EP = 64


def plant(values, rng, least, largest):
    index_at = [jax.random.randint(jax.random.fold_in(rng, axis), (), 0, length) for axis, length in enumerate(values.shape)]
    main_axis = values.shape.index(max(values.shape))
    beside = index_at[:main_axis] + [(index_at[main_axis] + 1) % values.shape[main_axis]] + index_at[main_axis + 1:]
    return values.at[tuple(index_at)].set(least).at[tuple(beside)].set(largest)


def level_of(stream_key, extent, pieces, least, high):
    gain = 1.0
    for position, parts in pieces:
        draws = jax.random.uniform(jax.random.fold_in(jax.random.fold_in(stream_key, 6), position), (parts,), jnp.float32, least / len(pieces), high / len(pieces))
        gain = gain * jnp.repeat(jnp.exp(draws), extent[position] // parts).reshape((-1,) + (1,) * (len(extent) - 1 - position))
    return gain


def deal_out(rng, own, number, rows, count, top, bound, slope):
    order = jax.random.permutation(rng, count)
    packed, common = portions_of(count, rows * top, bound, slope, True), portions_of(count, rows * top, bound, slope, False)
    places = jnp.arange(count)

    def named(tallies, rotation):
        used = int((tallies > 0).sum())
        fixed = max(1, used // 4)
        passed = fixed + (places - fixed + rotation * (used - fixed)) % max(1, count - fixed)
        return jnp.zeros((count,), jnp.int32).at[order[jnp.where(places < fixed, places, passed)]].set(jnp.asarray(tallies, jnp.int32))

    tallies = jnp.where(number % 4 == 0, named(packed, number // 4), named(common, number - number // 4 - 1))
    mixed = jax.random.permutation(jax.random.fold_in(own, 3), count)
    giver, taker = mixed[0:count // 2 * 2:2], mixed[1:count // 2 * 2:2]
    room = jnp.minimum(tallies[giver] - 1, bound - tallies[taker]) // 2
    room = jnp.where((giver == order[0]) | (taker == order[0]) | (tallies[taker] == 0), 0, jnp.maximum(room, 0))
    passed = jax.random.randint(jax.random.fold_in(own, 4), (count // 2,), 0, 1 << 20) % (room + 1)
    tallies = tallies.at[giver].add(-passed).at[taker].add(passed)
    labels = jnp.searchsorted(jnp.cumsum(tallies), jnp.arange(rows * top), side="right").astype(jnp.int32)
    listing = labels.reshape(top, rows).T
    listing = listing[jax.random.permutation(jax.random.fold_in(own, 1), rows)]
    rotation = jax.random.randint(jax.random.fold_in(own, 2), (rows, 1), 0, top)
    return jnp.take_along_axis(listing, (jnp.arange(top)[None, :] + rotation) % top, axis=1)


def portions_of(count, total, limit, skew, full):
    portions = [(1 << 20) // math.isqrt(grade ** skew) + 1 for grade in range(1, count + 1)]
    largest = limit if full else min(limit, max(-(-total // count), total * portions[0] // sum(portions)))
    least = 1 if total - largest >= count - 1 else 0
    counts, rest = [largest] + [least] * (count - 1), total - largest - least * (count - 1)
    while rest > 0:
        movable = [i for i in range(1, count) if counts[i] < largest] or [i for i in range(1, count) if counts[i] < limit]
        mass, left = sum([portions[i] for i in movable]), rest
        for i in movable:
            more = min(limit - counts[i], max(1, left * portions[i] // mass), rest)
            counts[i] = counts[i] + more
            rest = rest - more
    return np.array(counts)


def gaussian(key, extent, deviation, reach, cuts=(), kind=jnp.bfloat16):
    loudness = level_of(key, extent, cuts, -0.22, 0.18) if cuts else 1.0
    entries = jax.random.normal(key, extent, jnp.float32) * deviation * loudness
    return jnp.minimum(jnp.maximum(entries, -reach), reach).astype(kind)


def setup_inputs(seed: int = 0) -> dict:
    arg_keys = jax.random.split(jax.random.key(seed), 7)
    tokens = gaussian(arg_keys[0], (TOKENS, D), 1.0, 6.0, ((0, 64), (1, 16)))
    routes_keys = jax.random.split(jax.random.fold_in(arg_keys[1], 1), TOKENS // TOK_EP)
    routes_turns = jax.random.permutation(jax.random.fold_in(arg_keys[1], 3), TOKENS // TOK_EP)
    routes = jax.vmap(lambda own, number: deal_out(jax.random.fold_in(arg_keys[1], 2), own, number, TOK_EP, EXPERTS, TOP, CAP, 2))(routes_keys, routes_turns).reshape((TOKENS, TOP))
    gate_levels = plant(jax.random.randint(arg_keys[2], (TOKENS, TOP), 1, 256), jax.random.fold_in(arg_keys[2], 1), 1, 255).astype(jnp.int32)
    w_gate = gaussian(arg_keys[3], (EXPERTS, D, FF), D ** -0.5, 0.09375, ((0, 64), (1, 16)))
    w_up = gaussian(arg_keys[4], (EXPERTS, D, FF), D ** -0.5, 0.09375, ((0, 64), (1, 16)))
    w_down = gaussian(arg_keys[5], (EXPERTS, FF, D), FF ** -0.5, 0.1875, ((0, 64), (2, 16)))
    return {"tokens": tokens, "routes": routes, "gate_levels": gate_levels, "w_gate": w_gate, "w_up": w_up, "w_down": w_down}


def expert_apply(operands):
    inputs, gate_w, up_w, down_w = operands
    gate_act = jnp.dot(inputs, gate_w, preferred_element_type=jnp.float32)
    up_act = jnp.dot(inputs, up_w, preferred_element_type=jnp.float32)
    hidden = (jax.nn.silu(gate_act) * up_act).astype(jnp.bfloat16)
    return jnp.dot(hidden, down_w, preferred_element_type=jnp.float32).astype(jnp.bfloat16)


def reference(tokens, routes, gate_levels, w_gate, w_up, w_down):
    block_rows = TOK_EP * TOP
    flat_ids = routes.reshape(N_EP, block_rows).astype(jnp.int32)
    same_expert = flat_ids[:, :, None] == flat_ids[:, None, :]
    positions = jnp.arange(block_rows, dtype=jnp.int32)
    earlier = positions[:, None] > positions[None, :]
    slot_index = jnp.sum(same_expert & earlier[None], axis=2).astype(jnp.int32)
    block_ids = jnp.arange(N_EP, dtype=jnp.int32)[:, None]
    buffer_index = (flat_ids * (N_EP * CAP) + block_ids * CAP + slot_index).reshape(-1).astype(jnp.int32)
    owners = (jnp.arange(TOKENS * TOP, dtype=jnp.int32) // TOP).astype(jnp.int32)
    expert_rows = jnp.zeros((EXPERTS * N_EP * CAP, D), jnp.bfloat16).at[buffer_index].set(tokens[owners])
    expert_rows = expert_rows.reshape(EXPERTS, N_EP * CAP, D)
    expert_out = lax.map(expert_apply, (expert_rows, w_gate, w_up, w_down))
    picked = expert_out.reshape(EXPERTS * N_EP * CAP, D)[buffer_index].reshape(TOKENS, TOP, D).astype(jnp.float32)
    levels = gate_levels.astype(jnp.float32)
    weights = levels / jnp.sum(levels, axis=1, keepdims=True)
    return jnp.sum(weights[:, :, None] * picked, axis=1).astype(jnp.bfloat16)
```

```python
import functools

import jax
import jax.numpy as jnp
from jax import lax
from jax.experimental import pallas as pl
from jax.experimental.pallas import tpu as pltpu
from jax.sharding import PartitionSpec as P

NX, NY, NZ = 4, 8, 16
TOP = 8
CAP = 18
SLOT = 32
MESH = pl.DeviceIdType.MESH
F32 = jnp.float32
BF16 = jnp.bfloat16


def nn(a, b):
    return lax.dot_general(a, b, (((1,), (0,)), ((), ())), preferred_element_type=F32)


def nt(a, b):
    return lax.dot_general(a, b, (((1,), (1,)), ((), ())), preferred_element_type=F32)


def tn(a, b):
    return lax.dot_general(a, b, (((0,), (0,)), ((), ())), preferred_element_type=F32)


def kernel(
    tok_ref, routes_ref, levels_ref, wg_ref, wu_ref, wd_ref, out_ref,
    xb, cl, gs, gd, rx_own, rx_par, w_own, w_par, wd_own, wd_par,
    rs_out, rs_in, h_own, h_par, o_buf, rb, z_out, z_in,
    tok_sem, w_sem, wr_send, wr_recv, za_send, za_recv, xd_send, xd_recv,
    pr_send, pr_recv, rs_send, rs_recv, hy_send, hy_recv, hp_send, hp_recv,
    xr_send, xr_recv, zr_send, zr_recv,
):
    toks = tok_ref.shape[1]
    feats = tok_ref.shape[0]
    low = xb.shape[2]
    grp = NZ // 2
    rows = grp * CAP
    ff_half = w_own.shape[1] // 2
    hc = ff_half // 2
    quarter = NX and NY // 2
    experts = NX * NZ

    ep, tp = lax.axis_index("ep"), lax.axis_index("tp")
    x, z = ep // NZ, ep % NZ
    y, c = tp // 2, tp % 2

    def at_z(d):
        return (x * NZ + (z + d + NZ) % NZ, tp)

    def at_x(d):
        return (((x + d) % NX) * NZ + z, tp)

    def at_y(d):
        return (ep, ((y + d + NY) % NY) * 2 + c)

    partner = (ep, y * 2 + 1 - c)

    tok_a = pltpu.make_async_copy(tok_ref.at[pl.ds(0, low)], xb.at[0, 0], tok_sem.at[0])
    tok_b = pltpu.make_async_copy(
        tok_ref.at[pl.ds(low, feats - low)], xb.at[0, 1, pl.ds(0, feats - low)], tok_sem.at[1]
    )
    tok_a.start()
    tok_b.start()
    mine = pl.ds(pl.multiple_of(c * ff_half, ff_half), ff_half)
    other = pl.ds(pl.multiple_of((1 - c) * ff_half, ff_half), ff_half)
    w_local = [
        pltpu.make_async_copy(wg_ref.at[:, mine], w_own.at[:, pl.ds(0, ff_half)], w_sem.at[0]),
        pltpu.make_async_copy(wu_ref.at[:, mine], w_own.at[:, pl.ds(ff_half, ff_half)], w_sem.at[1]),
        pltpu.make_async_copy(wd_ref.at[:, mine], wd_own, w_sem.at[2]),
        pltpu.make_async_copy(wd_ref.at[:, other], wd_par, w_sem.at[3]),
    ]
    for copy in w_local:
        copy.start()

    barrier = pltpu.get_barrier_semaphore()
    for peer in [at_z(1), at_z(-1), at_y(1), at_y(-1), partner] + [at_x(d) for d in range(1, NX)]:
        pl.semaphore_signal(barrier, inc=1, device_id=peer, device_id_type=MESH)

    routes = routes_ref[...].astype(F32)
    levels = levels_ref[...].astype(F32)
    ids = lax.broadcasted_iota(jnp.int32, (experts, toks), 0).astype(F32)
    named = jnp.zeros((experts, toks), F32)
    for k in range(TOP):
        named = named + jnp.where(ids == routes[k : k + 1], 1.0, 0.0)
    before = (
        lax.broadcasted_iota(jnp.int32, (toks, toks), 0) < lax.broadcasted_iota(jnp.int32, (toks, toks), 1)
    ).astype(F32)
    count = nn(named.astype(BF16), before.astype(BF16))
    slots = [
        jnp.sum(jnp.where(ids == routes[k : k + 1], count, 0.0), axis=0, keepdims=True) for k in range(TOP)
    ]
    meta = jnp.concatenate([routes] + slots + [levels, jnp.zeros((8, toks), F32)], axis=0)
    tok_a.wait()
    tok_b.wait()
    xb[0, 1, feats - low :, :] = meta.astype(BF16)

    pl.semaphore_wait(barrier, 5 + NX - 1)

    w_remote = [
        pltpu.make_async_remote_copy(
            src_ref=wg_ref.at[:, other], dst_ref=w_par.at[:, pl.ds(0, ff_half)],
            send_sem=wr_send.at[0], recv_sem=wr_recv.at[0], device_id=partner, device_id_type=MESH,
        ),
        pltpu.make_async_remote_copy(
            src_ref=wu_ref.at[:, other], dst_ref=w_par.at[:, pl.ds(ff_half, ff_half)],
            send_sem=wr_send.at[1], recv_sem=wr_recv.at[1], device_id=partner, device_id_type=MESH,
        ),
    ]

    def z_copy(way, s, h):
        src = s - 1 if way == 0 else (NZ + 1 - s) % NZ
        dst = s if way == 0 else NZ - s
        return pltpu.make_async_remote_copy(
            src_ref=xb.at[src, h], dst_ref=xb.at[dst, h],
            send_sem=za_send.at[way, s, h], recv_sem=za_recv.at[way, s, h],
            device_id=at_z(1 if way == 0 else -1), device_id_type=MESH,
        )

    for h in range(2):
        for way in range(2):
            z_copy(way, 1, h).start()
    for copy in w_remote:
        copy.start()

    iota_slot = lax.broadcasted_iota(jnp.int32, (SLOT, toks), 0).astype(F32)

    def place(r):
        pos = (r + grp // 2 - 1) % NZ
        return pos // grp, pos % grp

    def select(r):
        g, pos = place(r)
        info = xb[r, 1, feats - low :, :].astype(F32)
        codes, shares = [], []
        for j in range(NX):
            hit = info[0:TOP] == (((x + j) % NX) * NZ + z).astype(F32)
            codes.append(jnp.sum(jnp.where(hit, info[TOP : 2 * TOP] + 1.0, 0.0), axis=0, keepdims=True) - 1.0)
            shares.append(jnp.sum(jnp.where(hit, info[2 * TOP : 3 * TOP], 0.0), axis=0, keepdims=True))
        cl[r] = jnp.concatenate(codes + shares, axis=0)
        pick = jnp.concatenate([jnp.where(iota_slot == code, 1.0, 0.0) for code in codes], axis=0).astype(BF16)
        for h in range(2):
            got = nt(pick, xb[r, h]).astype(BF16)
            for j in range(NX):
                gs[j, g, pl.ds(pl.multiple_of(pos * SLOT, SLOT), SLOT), h * low : (h + 1) * low] = got[
                    j * SLOT : (j + 1) * SLOT
                ]

    row = lax.broadcasted_iota(jnp.int32, (rows, grp * SLOT), 0)
    col = lax.broadcasted_iota(jnp.int32, (rows, grp * SLOT), 1)
    inside = col & (SLOT - 1)
    squeeze = jnp.where(((col >> 5) * CAP + inside == row) & (inside < CAP), 1.0, 0.0).astype(BF16)

    def xd_copy(j, g, q):
        return pltpu.make_async_remote_copy(
            src_ref=gd.at[j, g], dst_ref=rx_own.at[q], send_sem=xd_send.at[j, g], recv_sem=xd_recv.at[q],
            device_id=at_x(j), device_id_type=MESH,
        )

    def pr_copy(q):
        return pltpu.make_async_remote_copy(
            src_ref=rx_own.at[q], dst_ref=rx_par.at[q], send_sem=pr_send.at[q], recv_sem=pr_recv.at[q],
            device_id=partner, device_id_type=MESH,
        )

    def emit(g):
        for j in [*range(1, NX), 0]:
            packed = nn(squeeze, gs[j, g]).astype(BF16)
            if j:
                gd[j, g] = packed
                xd_copy(j, g, x * 2 + g).start()
            else:
                rx_own[x * 2 + g] = packed
                pr_copy(x * 2 + g).start()

    select(0)

    def z_step(s):
        for h in range(2):
            for way in range(2):
                z_copy(way, s, h).wait_recv()
                z_copy(way, s + 1, h).start()
        select(s)
        select(NZ - s)

    @pl.loop(1, grp // 2)
    def _(s):
        z_step(s)

    def late(s):
        for h in range(2):
            for way in range(2):
                z_copy(way, s, h).wait_recv()
                if way == 0 or s + 1 < grp:
                    z_copy(way, s + 1, h).start()

    late(grp // 2)
    select(grp // 2)
    emit(0)
    select(NZ - grp // 2)

    @pl.loop(grp // 2 + 1, grp - 1)
    def _(s):
        z_step(s)

    late(grp - 1)
    select(grp - 1)
    select(grp + 1)
    for g in range(1):
        for j in range(1, NX):
            q = ((x + NX - j) % NX) * 2 + g
            xd_copy(j, g, q).wait_recv()
            pr_copy(q).start()
    for h in range(2):
        z_copy(0, grp, h).wait_recv()
    select(grp)
    emit(1)
    for j in range(1, NX):
        q = ((x + NX - j) % NX) * 2 + 1
        xd_copy(j, 1, q).wait_recv()
        pr_copy(q).start()
    for copy in w_local:
        copy.wait()
    for copy in w_remote:
        copy.wait_recv()
    for q in range(NY):
        pr_copy(q).wait_recv()

    def part(q, p):
        cols = slice(p * ff_half, (p + 1) * ff_half)
        return nn(rx_own[q][:, :feats], w_own[:, cols]) + nn(rx_par[q][:, :feats], w_par[:, cols])

    half = NY // 2

    def rs_copy(way, d, p):
        return pltpu.make_async_remote_copy(
            src_ref=rs_out.at[way, d - 1, p], dst_ref=rs_in.at[way, d - 1, p],
            send_sem=rs_send.at[way, d - 1, p], recv_sem=rs_recv.at[way, d - 1, p],
            device_id=at_y(1 if way == 0 else -1), device_id_type=MESH,
        )

    def rs_step(way, d, p, takes):
        q = (y + d) % NY if way == 0 else (y + NY - d) % NY
        value = part(q, p)
        if takes:
            rs_copy(way, d + 1, p).wait_recv()
            value = value + rs_in[way, d, p].astype(F32)
        rs_out[way, d - 1, p] = value.astype(BF16)
        rs_copy(way, d, p).start()

    for way in range(2):
        rs_step(way, half, way, False)
    for way in range(2):
        rs_step(way, half - 1, 1 - way, False)
    for way in range(2):
        rs_step(way, half - 1, way, True)
    for d in range(half - 2, 0, -1):
        for p in range(2):
            for way in range(2):
                rs_step(way, d, (1 - way) if p == 0 else way, True)
    sums = []
    for p in range(2):
        value = part(y, p)
        for way in range(2):
            rs_copy(way, 1, p).wait_recv()
            value = value + rs_in[way, 0, p].astype(F32)
        sums.append(value)
    hidden = (sums[0] / (1.0 + jnp.exp(-sums[0])) * sums[1]).astype(BF16)
    for p in range(2):
        h_own[0, p] = hidden[:, p * hc : (p + 1) * hc]

    def hy_copy(way, d, p):
        src = d - 1 if way == 0 else (NY + 1 - d) % NY
        dst = d if way == 0 else NY - d
        return pltpu.make_async_remote_copy(
            src_ref=h_own.at[src, p], dst_ref=h_own.at[dst, p],
            send_sem=hy_send.at[way, d - 1, p], recv_sem=hy_recv.at[way, d - 1, p],
            device_id=at_y(1 if way == 0 else -1), device_id_type=MESH,
        )

    def hp_copy(r, p):
        return pltpu.make_async_remote_copy(
            src_ref=h_own.at[r, p], dst_ref=h_par.at[r, p], send_sem=hp_send.at[r, p],
            recv_sem=hp_recv.at[r, p], device_id=partner, device_id_type=MESH,
        )

    def xr_copy(r, i, g):
        return pltpu.make_async_remote_copy(
            src_ref=o_buf.at[r], dst_ref=rb.at[(NX - i) % NX, g], send_sem=xr_send.at[i, g],
            recv_sem=xr_recv.at[(NX - i) % NX, g], device_id=at_x(i), device_id_type=MESH,
        )

    def where_to(r):
        q = (y + NY - r) % NY
        return (q // 2 + NX - x) % NX, q % 2

    def down(r):
        acc = None
        for p in range(2):
            hp_copy(r, p).wait_recv()
        for p in range(2):
            cols = slice(p * hc, (p + 1) * hc)
            term = nt(h_own[r, p], wd_own[:, cols]) + nt(h_par[r, p], wd_par[:, cols])
            acc = term if acc is None else acc + term
        o_buf[r] = acc.astype(BF16)
        i, g = where_to(r)

        @pl.when(i != 0)
        def _():
            xr_copy(r, i, g).start()

        @pl.when(i == 0)
        def _():
            rb[0, g] = acc.astype(BF16)

    for p in range(2):
        for way in range(2):
            hy_copy(way, 1, p if way == 0 else 1 - p).start()
    for p in range(2):
        hp_copy(0, p).start()
    for d in range(1, half + 1):
        for p in range(2):
            for way in range(2):
                part_no = p if way == 0 else 1 - p
                if d == half and part_no != way:
                    continue
                hy_copy(way, d, part_no).wait_recv()
                if d + 1 < half or (d + 1 == half and part_no == way):
                    hy_copy(way, d + 1, part_no).start()
                hp_copy(d if way == 0 else NY - d, part_no).start()
        down(d - 1)
        if d > 1:
            down(NY - d + 1)
    down(half)

    for g in range(2):
        for j in range(1, NX):
            xr_copy(0, NX - j, g).wait_recv()

    iota_row = lax.broadcasted_iota(jnp.int32, (rows, toks), 0).astype(F32)
    zh = feats // 2

    def partial(r):
        g, pos = place(r)
        info = cl[r]
        base = (pos * CAP).astype(F32)
        acc = None
        for j in range(NX):
            code = info[j : j + 1]
            target = jnp.where(code >= 0.0, code + base, -1.0)
            mix = jnp.where(iota_row == target, info[NX + j : NX + j + 1], 0.0).astype(BF16)
            term = tn(rb[j, g], mix)
            acc = term if acc is None else acc + term
        return acc

    def zr_copy(way, d, h):
        return pltpu.make_async_remote_copy(
            src_ref=z_out.at[way, d - 1, h], dst_ref=z_in.at[way, d - 1, h],
            send_sem=zr_send.at[way, d - 1, h], recv_sem=zr_recv.at[way, d - 1, h],
            device_id=at_z(1 if way == 0 else -1), device_id_type=MESH,
        )

    def zr_step(d, takes):
        values = [(way, partial(jnp.asarray(NZ - d if way == 0 else d, jnp.int32))) for way in takes]
        for h in range(2):
            for way, value in values:
                piece = value[h * zh : (h + 1) * zh]
                if takes[way]:
                    zr_copy(way, d + 1, h).wait_recv()
                    piece = piece + z_in[way, d, h].astype(F32)
                z_out[way, d - 1, h] = piece.astype(BF16)
                zr_copy(way, d, h).start()

    zr_step(grp, {0: False})
    zr_step(grp - 1, {0: True, 1: False})

    @pl.loop(0, grp - 2)
    def _(t):
        zr_step(grp - 2 - t, {0: True, 1: True})

    total = partial(jnp.asarray(0, jnp.int32))
    scale = jnp.sum(levels, axis=0, keepdims=True)
    for h in range(2):
        piece = total[h * zh : (h + 1) * zh]
        for way in range(2):
            zr_copy(way, 1, h).wait_recv()
            piece = piece + z_in[way, 0, h].astype(F32)
        out_ref[h * zh : (h + 1) * zh, :] = (piece / scale).astype(BF16)

    for copy in w_remote:
        copy.wait_send()
    for way in range(2):
        for h in range(2):

            @pl.loop(1, grp + 1 - way)
            def _(s, way=way, h=h):
                z_copy(way, s, h).wait_send()
                zr_copy(way, s, h).wait_send()

    for g in range(2):
        for j in range(1, NX):
            xd_copy(j, g, 0).wait_send()
            xr_copy(0, j, g).wait_send()
    for r in range(NY):
        pr_copy(r).wait_send()
        for p in range(2):
            hp_copy(r, p).wait_send()
    for way in range(2):
        for d in range(1, half + 1):
            for p in range(2):
                if d < half or p == way:
                    rs_copy(way, d, p).wait_send()
                    hy_copy(way, d, p).wait_send()


def on_device(tokens, routes, gate_levels, w_gate, w_up, w_down):
    toks, feats = tokens.shape
    ff = w_gate.shape[2]
    low = 128
    grp = NZ // 2
    rows = grp * CAP
    half = NY // 2
    dma = pltpu.SemaphoreType.DMA
    out = pl.pallas_call(
        kernel,
        out_shape=jax.ShapeDtypeStruct((feats, toks), BF16),
        in_specs=[pl.BlockSpec(memory_space=pl.ANY)]
        + [pl.BlockSpec(memory_space=pltpu.VMEM)] * 2
        + [pl.BlockSpec(memory_space=pl.ANY)] * 3,
        out_specs=pl.BlockSpec(memory_space=pltpu.VMEM),
        scratch_shapes=[
            pltpu.VMEM((NZ, 2, low, toks), BF16),
            pltpu.VMEM((NZ, 2 * NX, toks), F32),
            pltpu.VMEM((NX, 2, grp * SLOT, 2 * low), BF16),
            pltpu.VMEM((NX, 2, rows, 2 * low), BF16),
            pltpu.VMEM((NY, rows, 2 * low), BF16),
            pltpu.VMEM((NY, rows, 2 * low), BF16),
            pltpu.VMEM((feats, ff), BF16),
            pltpu.VMEM((feats, ff), BF16),
            pltpu.VMEM((feats, ff // 2), BF16),
            pltpu.VMEM((feats, ff // 2), BF16),
            pltpu.VMEM((2, half, 2, rows, ff // 2), BF16),
            pltpu.VMEM((2, half, 2, rows, ff // 2), BF16),
            pltpu.VMEM((NY, 2, rows, ff // 4), BF16),
            pltpu.VMEM((NY, 2, rows, ff // 4), BF16),
            pltpu.VMEM((NY, rows, feats), BF16),
            pltpu.VMEM((NX, 2, rows, feats), BF16),
            pltpu.VMEM((2, grp, 2, feats // 2, toks), BF16),
            pltpu.VMEM((2, grp, 2, feats // 2, toks), BF16),
            dma((2,)), dma((4,)), dma((2,)), dma((2,)),
            dma((2, grp + 1, 2)), dma((2, grp + 1, 2)),
            dma((NX, 2)), dma((NY,)),
            dma((NY,)), dma((NY,)),
            dma((2, half, 2)), dma((2, half, 2)),
            dma((2, half, 2)), dma((2, half, 2)),
            dma((NY, 2)), dma((NY, 2)),
            dma((NX, 2)), dma((NX, 2)),
            dma((2, grp, 2)), dma((2, grp, 2)),
        ],
        compiler_params=pltpu.CompilerParams(
            collective_id=0, has_side_effects=True, vmem_limit_bytes=60 * 1024 * 1024
        ),
    )(
        tokens.T, routes.T, gate_levels.T,
        w_gate.reshape(feats, ff), w_up.reshape(feats, ff), w_down.reshape(ff, feats).T,
    )
    return out.T


def solution(mesh):
    in_specs = (
        P("ep", "tp"),
        P("ep", None),
        P("ep", None),
        P("ep", "tp", None),
        P("ep", "tp", None),
        P("ep", None, "tp"),
    )
    out_specs = P("ep", "tp")
    return jax.shard_map(
        on_device, mesh=mesh, in_specs=in_specs, out_specs=out_specs, check_vma=False
    )
```

```python
import functools

import jax
import jax.numpy as jnp
from jax import lax
from jax.experimental import pallas as pl
from jax.experimental.pallas import tpu as pltpu
from jax.sharding import PartitionSpec as P

NX, NY, NZ = 4, 8, 16
TOP = 8
CAP = 18
SLOT = 32
MESH = pl.DeviceIdType.MESH
F32 = jnp.float32
BF16 = jnp.bfloat16


def nn(a, b):
    return lax.dot_general(a, b, (((1,), (0,)), ((), ())), preferred_element_type=F32)


def nt(a, b):
    return lax.dot_general(a, b, (((1,), (1,)), ((), ())), preferred_element_type=F32)


def tn(a, b):
    return lax.dot_general(a, b, (((0,), (0,)), ((), ())), preferred_element_type=F32)


def kernel(
    tok_ref, routes_ref, levels_ref, wg_ref, wu_ref, wd_ref, out_ref,
    xb, cl, gs, gd, rx_own, rx_par, w_own, w_par, wd_own, wd_par,
    rs_out, rs_in, h_own, h_par, o_buf, rb, z_out, z_in,
    tok_sem, w_sem, wr_send, wr_recv, za_send, za_recv, xd_send, xd_recv,
    pr_send, pr_recv, rs_send, rs_recv, hy_send, hy_recv, hp_send, hp_recv,
    xr_send, xr_recv, zr_send, zr_recv,
):
    toks = tok_ref.shape[1]
    feats = tok_ref.shape[0]
    low = xb.shape[2]
    grp = NZ // 2
    rows = grp * CAP
    hc = h_own.shape[4]
    ff_half = hc * 4
    experts = NX * NZ

    ep, tp = lax.axis_index("ep"), lax.axis_index("tp")
    x, z = ep // NZ, ep % NZ
    y, c = tp // 2, tp % 2

    def at_z(d):
        return (x * NZ + (z + d + NZ) % NZ, tp)

    def at_x(d):
        return (((x + d) % NX) * NZ + z, tp)

    def at_y(d):
        return (ep, ((y + d + NY) % NY) * 2 + c)

    partner = (ep, y * 2 + 1 - c)

    tok_a = pltpu.make_async_copy(tok_ref.at[pl.ds(0, low)], xb.at[0, 0], tok_sem.at[0])
    tok_b = pltpu.make_async_copy(
        tok_ref.at[pl.ds(low, feats - low)], xb.at[0, 1, pl.ds(0, feats - low)], tok_sem.at[1]
    )
    tok_a.start()
    tok_b.start()
    mine = pl.ds(pl.multiple_of(c * ff_half, ff_half), ff_half)
    other = pl.ds(pl.multiple_of((1 - c) * ff_half, ff_half), ff_half)
    def cols_of(core, ch):
        return pl.ds(pl.multiple_of(core * ff_half + ch * 2 * hc, 2 * hc), 2 * hc)

    w_local = [
        pltpu.make_async_copy(w.at[:, cols_of(c, ch)], w_own.at[p, ch], w_sem.at[p * 2 + ch])
        for p, w in enumerate((wg_ref, wu_ref))
        for ch in range(2)
    ] + [
        pltpu.make_async_copy(wd_ref.at[:, mine], wd_own, w_sem.at[4]),
        pltpu.make_async_copy(wd_ref.at[:, other], wd_par, w_sem.at[5]),
    ]
    for copy in w_local:
        copy.start()

    barrier = pltpu.get_barrier_semaphore()
    for peer in [at_z(1), at_z(-1), at_y(1), at_y(-1), partner] + [at_x(d) for d in range(1, NX)]:
        pl.semaphore_signal(barrier, inc=1, device_id=peer, device_id_type=MESH)

    routes = routes_ref[...].astype(F32)
    levels = levels_ref[...].astype(F32)
    ids = lax.broadcasted_iota(jnp.int32, (experts, toks), 0).astype(F32)
    named = jnp.zeros((experts, toks), F32)
    for k in range(TOP):
        named = named + jnp.where(ids == routes[k : k + 1], 1.0, 0.0)
    before = (
        lax.broadcasted_iota(jnp.int32, (toks, toks), 0) < lax.broadcasted_iota(jnp.int32, (toks, toks), 1)
    ).astype(F32)
    count = nn(named.astype(BF16), before.astype(BF16))
    slots = [
        jnp.sum(jnp.where(ids == routes[k : k + 1], count, 0.0), axis=0, keepdims=True) for k in range(TOP)
    ]
    meta = jnp.concatenate([routes] + slots + [levels, jnp.zeros((8, toks), F32)], axis=0)
    tok_a.wait()
    tok_b.wait()
    xb[0, 1, feats - low :, :] = meta.astype(BF16)

    pl.semaphore_wait(barrier, 5 + NX - 1)

    w_remote = [
        pltpu.make_async_remote_copy(
            src_ref=w.at[:, cols_of(1 - c, ch)], dst_ref=w_par.at[p, ch],
            send_sem=wr_send.at[p * 2 + ch], recv_sem=wr_recv.at[p * 2 + ch],
            device_id=partner, device_id_type=MESH,
        )
        for p, w in enumerate((wg_ref, wu_ref))
        for ch in range(2)
    ]

    def z_copy(way, s, h):
        src = s - 1 if way == 0 else (NZ + 1 - s) % NZ
        dst = s if way == 0 else NZ - s
        return pltpu.make_async_remote_copy(
            src_ref=xb.at[src, h], dst_ref=xb.at[dst, h],
            send_sem=za_send.at[way, s, h], recv_sem=za_recv.at[way, s, h],
            device_id=at_z(1 if way == 0 else -1), device_id_type=MESH,
        )

    for h in range(2):
        for way in range(2):
            z_copy(way, 1, h).start()
    for copy in w_remote:
        copy.start()

    iota_slot = lax.broadcasted_iota(jnp.int32, (SLOT, toks), 0).astype(F32)

    def place(r):
        pos = (r + grp // 2 - 1) % NZ
        return pos // grp, pos % grp

    def select(r):
        g, pos = place(r)
        info = xb[r, 1, feats - low :, :].astype(F32)
        codes, shares = [], []
        for j in range(NX):
            hit = info[0:TOP] == (((x + j) % NX) * NZ + z).astype(F32)
            codes.append(jnp.sum(jnp.where(hit, info[TOP : 2 * TOP] + 1.0, 0.0), axis=0, keepdims=True) - 1.0)
            shares.append(jnp.sum(jnp.where(hit, info[2 * TOP : 3 * TOP], 0.0), axis=0, keepdims=True))
        cl[r] = jnp.concatenate(codes + shares, axis=0)
        pick = jnp.concatenate([jnp.where(iota_slot == code, 1.0, 0.0) for code in codes], axis=0).astype(BF16)
        for h in range(2):
            got = nt(pick, xb[r, h]).astype(BF16)
            for j in range(NX):
                gs[j, g, pl.ds(pl.multiple_of(pos * SLOT, SLOT), SLOT), h * low : (h + 1) * low] = got[
                    j * SLOT : (j + 1) * SLOT
                ]

    row = lax.broadcasted_iota(jnp.int32, (rows, grp * SLOT), 0)
    col = lax.broadcasted_iota(jnp.int32, (rows, grp * SLOT), 1)
    inside = col & (SLOT - 1)
    squeeze = jnp.where(((col >> 5) * CAP + inside == row) & (inside < CAP), 1.0, 0.0).astype(BF16)

    def xd_copy(j, g, q):
        return pltpu.make_async_remote_copy(
            src_ref=gd.at[j, g], dst_ref=rx_own.at[q], send_sem=xd_send.at[j, g], recv_sem=xd_recv.at[q],
            device_id=at_x(j), device_id_type=MESH,
        )

    def pr_copy(q):
        return pltpu.make_async_remote_copy(
            src_ref=rx_own.at[q], dst_ref=rx_par.at[q], send_sem=pr_send.at[q], recv_sem=pr_recv.at[q],
            device_id=partner, device_id_type=MESH,
        )

    def emit(g):
        for j in [*range(1, NX), 0]:
            packed = nn(squeeze, gs[j, g]).astype(BF16)
            if j:
                gd[j, g] = packed
                xd_copy(j, g, x * 2 + g).start()
            else:
                rx_own[x * 2 + g] = packed
                pr_copy(x * 2 + g).start()

    select(0)

    def z_step(s):
        for h in range(2):
            for way in range(2):
                z_copy(way, s, h).wait_recv()
                z_copy(way, s + 1, h).start()
        select(s)
        select(NZ - s)

    @pl.loop(1, grp // 2)
    def _(s):
        z_step(s)

    def late(s):
        for h in range(2):
            for way in range(2):
                if way == 0 or s < grp:
                    z_copy(way, s, h).wait_recv()
                if s + 1 < grp or (way == 0 and s + 1 == grp):
                    z_copy(way, s + 1, h).start()

    def arrive(g):
        for j in range(1, NX):
            q = ((x + NX - j) % NX) * 2 + g
            xd_copy(j, g, q).wait_recv()
            pr_copy(q).start()

    def arrive_partner(g):
        for j in range(NX):
            pr_copy(j * 2 + g).wait_recv()

    half = NY // 2

    def part(g, q, p):
        n, ch = (q // 2) * 2 + g, q % 2
        return nn(rx_own[n][:, :feats], w_own[p, ch]) + nn(rx_par[n][:, :feats], w_par[p, ch])

    def rs_copy(g, way, d, p):
        return pltpu.make_async_remote_copy(
            src_ref=rs_out.at[g, way, d - 1, p], dst_ref=rs_in.at[g, way, d - 1, p],
            send_sem=rs_send.at[g, way, d - 1, p], recv_sem=rs_recv.at[g, way, d - 1, p],
            device_id=at_y(1 if way == 0 else -1), device_id_type=MESH,
        )

    def rs_step(g, way, d, p):
        q = (y + d) % NY if way == 0 else (y + NY - d) % NY
        value = part(g, q, p)
        if d + 1 < half or (d + 1 == half and p == way):
            rs_copy(g, way, d + 1, p).wait_recv()
            value = value + rs_in[g, way, d, p].astype(F32)
        rs_out[g, way, d - 1, p] = value.astype(BF16)
        rs_copy(g, way, d, p).start()

    def rs_pair(g, d, late_half):
        for way in range(2):
            rs_step(g, way, d, way if late_half else 1 - way)

    def rs_first(g):
        rs_pair(g, half, True)
        rs_pair(g, half - 1, False)

    def rs_last(g):
        sums = []
        for p in range(2):
            value = part(g, y, p)
            for way in range(2):
                rs_copy(g, way, 1, p).wait_recv()
                value = value + rs_in[g, way, 0, p].astype(F32)
            sums.append(value)
        hidden = (sums[0] / (1.0 + jnp.exp(-sums[0])) * sums[1]).astype(BF16)
        for p in range(2):
            h_own[g, y, p] = hidden[:, p * hc : (p + 1) * hc]

    def hy_copy(g, way, d, p, q):
        return pltpu.make_async_remote_copy(
            src_ref=h_own.at[g, q, p], dst_ref=h_own.at[g, q, p],
            send_sem=hy_send.at[g, way, d - 1, p], recv_sem=hy_recv.at[g, way, d - 1, p],
            device_id=at_y(1 if way == 0 else -1), device_id_type=MESH,
        )

    def hp_copy(g, q):
        return pltpu.make_async_remote_copy(
            src_ref=h_own.at[g, q], dst_ref=h_par.at[g, q], send_sem=hp_send.at[g, q],
            recv_sem=hp_recv.at[g, q], device_id=partner, device_id_type=MESH,
        )

    def from_y(way, d):
        return (y + NY - d) % NY if way == 0 else (y + d) % NY

    def xr_copy(g, n, i):
        return pltpu.make_async_remote_copy(
            src_ref=o_buf.at[g, n], dst_ref=rb.at[(NX - i) % NX, g], send_sem=xr_send.at[i, g],
            recv_sem=xr_recv.at[(NX - i) % NX, g], device_id=at_x(i), device_id_type=MESH,
        )

    def down(g, step):
        turn = 1 - 2 * (y % 2)
        n = (y // 2 + NX + (0, -turn, turn, 2)[step]) % NX
        acc = None
        for ch in range(2):
            q = n * 2 + ch
            hp_copy(g, q).wait_recv()
            own = jnp.concatenate([h_own[g, q, 0], h_own[g, q, 1]], axis=1)
            par = jnp.concatenate([h_par[g, q, 0], h_par[g, q, 1]], axis=1)
            cols = slice(ch * 2 * hc, (ch + 1) * 2 * hc)
            term = nt(own, wd_own[:, cols]) + nt(par, wd_par[:, cols])
            acc = term if acc is None else acc + term
        o_buf[g, n] = acc.astype(BF16)
        i = (n + NX - x) % NX

        @pl.when(i != 0)
        def _():
            xr_copy(g, n, i).start()

        @pl.when(i == 0)
        def _():
            rb[0, g] = acc.astype(BF16)

    def ag_first(g):
        for p in range(2):
            for way in range(2):
                hy_copy(g, way, 1, p if way == 0 else 1 - p, y).start()
        hp_copy(g, y).start()

    def ag_step(g, d):
        for p in range(2):
            for way in range(2):
                part_no = p if way == 0 else 1 - p
                if d == half and part_no != way:
                    continue
                q = from_y(way, d)
                hy_copy(g, way, d, part_no, q).wait_recv()
                if d + 1 < half or (d + 1 == half and part_no == way):
                    hy_copy(g, way, d + 1, part_no, q).start()
        if d < half:
            for way in range(2):
                hp_copy(g, from_y(way, d)).start()
        else:
            hp_copy(g, from_y(0, d)).start()

    late(grp // 2)
    select(grp // 2)
    emit(0)
    select(NZ - grp // 2)
    late(grp // 2 + 1)
    select(grp // 2 + 1)
    select(NZ - grp // 2 - 1)
    arrive(0)
    late(grp // 2 + 2)
    for copy in w_local:
        copy.wait()
    for copy in w_remote:
        copy.wait_recv()
    arrive_partner(0)
    rs_first(0)
    select(grp - 2)
    select(grp + 2)
    late(grp - 1)
    rs_pair(0, half - 1, True)
    select(grp - 1)
    select(grp + 1)
    rs_pair(0, half - 2, False)
    late(grp)
    select(grp)
    emit(1)
    rs_pair(0, half - 2, True)
    rs_pair(0, half - 3, False)
    arrive(1)
    rs_pair(0, half - 3, True)
    arrive_partner(1)
    rs_first(1)
    rs_last(0)
    rs_pair(1, half - 1, True)
    rs_pair(1, half - 2, False)
    rs_pair(1, half - 2, True)
    rs_pair(1, half - 3, False)
    rs_pair(1, half - 3, True)
    ag_first(0)
    rs_last(1)
    ag_first(1)
    for d in range(1, half + 1):
        ag_step(0, d)
        ag_step(1, d)
        if d > 1:
            down(1, d - 2)
            down(0, d - 2)
    down(1, half - 1)
    down(0, half - 1)

    for g in range(2):
        for j in range(1, NX):
            xr_copy(g, 0, NX - j).wait_recv()

    iota_row = lax.broadcasted_iota(jnp.int32, (rows, toks), 0).astype(F32)
    zh = feats // 2

    def partial(r):
        g, pos = place(r)
        info = cl[r]
        base = (pos * CAP).astype(F32)
        acc = None
        for j in range(NX):
            code = info[j : j + 1]
            target = jnp.where(code >= 0.0, code + base, -1.0)
            mix = jnp.where(iota_row == target, info[NX + j : NX + j + 1], 0.0).astype(BF16)
            term = tn(rb[j, g], mix)
            acc = term if acc is None else acc + term
        return acc

    def zr_copy(way, d, h):
        return pltpu.make_async_remote_copy(
            src_ref=z_out.at[way, d - 1, h], dst_ref=z_in.at[way, d - 1, h],
            send_sem=zr_send.at[way, d - 1, h], recv_sem=zr_recv.at[way, d - 1, h],
            device_id=at_z(1 if way == 0 else -1), device_id_type=MESH,
        )

    def zr_step(d, takes):
        values = [(way, partial(jnp.asarray(NZ - d if way == 0 else d, jnp.int32))) for way in takes]
        for h in range(2):
            for way, value in values:
                piece = value[h * zh : (h + 1) * zh]
                if takes[way]:
                    zr_copy(way, d + 1, h).wait_recv()
                    piece = piece + z_in[way, d, h].astype(F32)
                z_out[way, d - 1, h] = piece.astype(BF16)
                zr_copy(way, d, h).start()

    zr_step(grp, {0: False})
    zr_step(grp - 1, {0: True, 1: False})

    @pl.loop(0, grp - 2)
    def _(t):
        zr_step(grp - 2 - t, {0: True, 1: True})

    total = partial(jnp.asarray(0, jnp.int32))
    scale = jnp.sum(levels, axis=0, keepdims=True)
    for h in range(2):
        piece = total[h * zh : (h + 1) * zh]
        for way in range(2):
            zr_copy(way, 1, h).wait_recv()
            piece = piece + z_in[way, 0, h].astype(F32)
        out_ref[h * zh : (h + 1) * zh, :] = (piece / scale).astype(BF16)

    for copy in w_remote:
        copy.wait_send()
    for way in range(2):
        for h in range(2):

            @pl.loop(1, grp + 1 - way)
            def _(s, way=way, h=h):
                z_copy(way, s, h).wait_send()
                zr_copy(way, s, h).wait_send()

    for g in range(2):
        for j in range(1, NX):
            xd_copy(j, g, 0).wait_send()
            xr_copy(g, 0, j).wait_send()
        for q in range(NY):
            hp_copy(g, q).wait_send()
        for way in range(2):
            for d in range(1, half + 1):
                for p in range(2):
                    if d < half or p == way:
                        rs_copy(g, way, d, p).wait_send()
                        hy_copy(g, way, d, p, 0).wait_send()
    for q in range(NY):
        pr_copy(q).wait_send()


def on_device(tokens, routes, gate_levels, w_gate, w_up, w_down):
    toks, feats = tokens.shape
    ff = w_gate.shape[2]
    low = 128
    grp = NZ // 2
    rows = grp * CAP
    half = NY // 2
    dma = pltpu.SemaphoreType.DMA
    out = pl.pallas_call(
        kernel,
        out_shape=jax.ShapeDtypeStruct((feats, toks), BF16),
        in_specs=[pl.BlockSpec(memory_space=pl.ANY)]
        + [pl.BlockSpec(memory_space=pltpu.VMEM)] * 2
        + [pl.BlockSpec(memory_space=pl.ANY)] * 3,
        out_specs=pl.BlockSpec(memory_space=pltpu.VMEM),
        scratch_shapes=[
            pltpu.VMEM((NZ, 2, low, toks), BF16),
            pltpu.VMEM((NZ, 2 * NX, toks), F32),
            pltpu.VMEM((NX, 2, grp * SLOT, 2 * low), BF16),
            pltpu.VMEM((NX, 2, rows, 2 * low), BF16),
            pltpu.VMEM((NY, rows, 2 * low), BF16),
            pltpu.VMEM((NY, rows, 2 * low), BF16),
            pltpu.VMEM((2, 2, feats, ff // 4), BF16),
            pltpu.VMEM((2, 2, feats, ff // 4), BF16),
            pltpu.VMEM((feats, ff // 2), BF16),
            pltpu.VMEM((feats, ff // 2), BF16),
            pltpu.VMEM((2, 2, half, 2, rows, ff // 4), BF16),
            pltpu.VMEM((2, 2, half, 2, rows, ff // 4), BF16),
            pltpu.VMEM((2, NY, 2, rows, ff // 8), BF16),
            pltpu.VMEM((2, NY, 2, rows, ff // 8), BF16),
            pltpu.VMEM((2, NX, rows, feats), BF16),
            pltpu.VMEM((NX, 2, rows, feats), BF16),
            pltpu.VMEM((2, grp, 2, feats // 2, toks), BF16),
            pltpu.VMEM((2, grp, 2, feats // 2, toks), BF16),
            dma((2,)), dma((6,)), dma((4,)), dma((4,)),
            dma((2, grp + 1, 2)), dma((2, grp + 1, 2)),
            dma((NX, 2)), dma((NY,)),
            dma((NY,)), dma((NY,)),
            dma((2, 2, half, 2)), dma((2, 2, half, 2)),
            dma((2, 2, half, 2)), dma((2, 2, half, 2)),
            dma((2, NY)), dma((2, NY)),
            dma((NX, 2)), dma((NX, 2)),
            dma((2, grp, 2)), dma((2, grp, 2)),
        ],
        compiler_params=pltpu.CompilerParams(
            collective_id=0, has_side_effects=True, vmem_limit_bytes=60 * 1024 * 1024
        ),
    )(
        tokens.T, routes.T, gate_levels.T,
        w_gate.reshape(feats, ff), w_up.reshape(feats, ff), w_down.reshape(ff, feats).T,
    )
    return out.T


def solution(mesh):
    in_specs = (
        P("ep", "tp"),
        P("ep", None),
        P("ep", None),
        P("ep", "tp", None),
        P("ep", "tp", None),
        P("ep", None, "tp"),
    )
    out_specs = P("ep", "tp")
    return jax.shard_map(
        on_device, mesh=mesh, in_specs=in_specs, out_specs=out_specs, check_vma=False
    )
```

```python
import functools

import jax
import jax.numpy as jnp
from jax import lax
from jax.experimental import pallas as pl
from jax.experimental.pallas import tpu as pltpu
from jax.sharding import PartitionSpec as P

NX, NY, NZ = 4, 8, 16
TOP = 8
CAP = 18
SLOT = 32
MESH = pl.DeviceIdType.MESH
F32 = jnp.float32
BF16 = jnp.bfloat16


def nn(a, b):
    return lax.dot_general(a, b, (((1,), (0,)), ((), ())), preferred_element_type=F32)


def nt(a, b):
    return lax.dot_general(a, b, (((1,), (1,)), ((), ())), preferred_element_type=F32)


def tn(a, b):
    return lax.dot_general(a, b, (((0,), (0,)), ((), ())), preferred_element_type=F32)


def kernel(
    tok_ref, routes_ref, levels_ref, wg_ref, wu_ref, wd_ref, out_ref,
    xb, cl, gs, gd, rx_own, rx_par, w_own, w_par, wd_own, wd_par,
    rs_out, rs_in, h_own, h_par, o_buf, rb, z_out, z_in,
    tok_sem, w_sem, wr_send, wr_recv, za_send, za_recv, xd_send, xd_recv,
    pr_send, pr_recv, rs_send, rs_recv, hy_send, hy_recv, hp_send, hp_recv,
    xr_send, xr_recv, zr_send, zr_recv,
):
    toks = tok_ref.shape[1]
    feats = tok_ref.shape[0]
    low = xb.shape[2]
    grp = NZ // 2
    rows = grp * CAP
    hc = h_own.shape[4]
    ff_half = hc * 4
    experts = NX * NZ

    ep, tp = lax.axis_index("ep"), lax.axis_index("tp")
    x, z = ep // NZ, ep % NZ
    y, c = tp // 2, tp % 2

    def at_z(d):
        return (x * NZ + (z + d + NZ) % NZ, tp)

    def at_x(d):
        return (((x + d) % NX) * NZ + z, tp)

    def at_y(d):
        return (ep, ((y + d + NY) % NY) * 2 + c)

    partner = (ep, y * 2 + 1 - c)

    tok_a = pltpu.make_async_copy(tok_ref.at[pl.ds(0, low)], xb.at[0, 0], tok_sem.at[0])
    tok_b = pltpu.make_async_copy(
        tok_ref.at[pl.ds(low, feats - low)], xb.at[0, 1, pl.ds(0, feats - low)], tok_sem.at[1]
    )
    tok_a.start()
    tok_b.start()
    mine = pl.ds(pl.multiple_of(c * ff_half, ff_half), ff_half)
    other = pl.ds(pl.multiple_of((1 - c) * ff_half, ff_half), ff_half)
    def cols_of(core, ch):
        return pl.ds(pl.multiple_of(core * ff_half + ch * 2 * hc, 2 * hc), 2 * hc)

    w_local = [
        pltpu.make_async_copy(w.at[:, cols_of(c, ch)], w_own.at[p, ch], w_sem.at[p * 2 + ch])
        for p, w in enumerate((wg_ref, wu_ref))
        for ch in range(2)
    ] + [
        pltpu.make_async_copy(wd_ref.at[:, mine], wd_own, w_sem.at[4]),
        pltpu.make_async_copy(wd_ref.at[:, other], wd_par, w_sem.at[5]),
    ]
    for copy in w_local:
        copy.start()

    barrier = pltpu.get_barrier_semaphore()
    for peer in [at_z(1), at_z(-1), at_y(1), at_y(-1), partner] + [at_x(d) for d in range(1, NX)]:
        pl.semaphore_signal(barrier, inc=1, device_id=peer, device_id_type=MESH)

    routes = routes_ref[...].astype(F32)
    levels = levels_ref[...].astype(F32)
    ids = lax.broadcasted_iota(jnp.int32, (experts, toks), 0).astype(F32)
    named = jnp.zeros((experts, toks), F32)
    for k in range(TOP):
        named = named + jnp.where(ids == routes[k : k + 1], 1.0, 0.0)
    before = (
        lax.broadcasted_iota(jnp.int32, (toks, toks), 0) < lax.broadcasted_iota(jnp.int32, (toks, toks), 1)
    ).astype(F32)
    count = nn(named.astype(BF16), before.astype(BF16))
    slots = [
        jnp.sum(jnp.where(ids == routes[k : k + 1], count, 0.0), axis=0, keepdims=True) for k in range(TOP)
    ]
    meta = jnp.concatenate([routes] + slots + [levels, jnp.zeros((8, toks), F32)], axis=0)
    tok_a.wait()
    tok_b.wait()
    xb[0, 1, feats - low :, :] = meta.astype(BF16)

    pl.semaphore_wait(barrier, 5 + NX - 1)

    w_remote = [
        pltpu.make_async_remote_copy(
            src_ref=w.at[:, cols_of(1 - c, ch)], dst_ref=w_par.at[p, ch],
            send_sem=wr_send.at[p * 2 + ch], recv_sem=wr_recv.at[p * 2 + ch],
            device_id=partner, device_id_type=MESH,
        )
        for p, w in enumerate((wg_ref, wu_ref))
        for ch in range(2)
    ]

    def z_copy(way, s, h):
        src = s - 1 if way == 0 else (NZ + 1 - s) % NZ
        dst = s if way == 0 else NZ - s
        return pltpu.make_async_remote_copy(
            src_ref=xb.at[src, h], dst_ref=xb.at[dst, h],
            send_sem=za_send.at[way, s, h], recv_sem=za_recv.at[way, s, h],
            device_id=at_z(1 if way == 0 else -1), device_id_type=MESH,
        )

    for h in range(2):
        for way in range(2):
            z_copy(way, 1, h).start()
    for copy in w_remote:
        copy.start()

    iota_slot = lax.broadcasted_iota(jnp.int32, (SLOT, toks), 0).astype(F32)

    def place(r):
        pos = (r + grp // 2 - 1) % NZ
        return pos // grp, pos % grp

    def select(r):
        g, pos = place(r)
        info = xb[r, 1, feats - low :, :].astype(F32)
        codes, shares = [], []
        for j in range(NX):
            hit = info[0:TOP] == (((x + j) % NX) * NZ + z).astype(F32)
            codes.append(jnp.sum(jnp.where(hit, info[TOP : 2 * TOP] + 1.0, 0.0), axis=0, keepdims=True) - 1.0)
            shares.append(jnp.sum(jnp.where(hit, info[2 * TOP : 3 * TOP], 0.0), axis=0, keepdims=True))
        cl[r] = jnp.concatenate(codes + shares, axis=0)
        pick = jnp.concatenate([jnp.where(iota_slot == code, 1.0, 0.0) for code in codes], axis=0).astype(BF16)
        for h in range(2):
            got = nt(pick, xb[r, h]).astype(BF16)
            for j in range(NX):
                gs[j, g, pl.ds(pl.multiple_of(pos * SLOT, SLOT), SLOT), h * low : (h + 1) * low] = got[
                    j * SLOT : (j + 1) * SLOT
                ]

    row = lax.broadcasted_iota(jnp.int32, (rows, grp * SLOT), 0)
    col = lax.broadcasted_iota(jnp.int32, (rows, grp * SLOT), 1)
    inside = col & (SLOT - 1)
    squeeze = jnp.where(((col >> 5) * CAP + inside == row) & (inside < CAP), 1.0, 0.0).astype(BF16)

    def xd_copy(j, g, q):
        return pltpu.make_async_remote_copy(
            src_ref=gd.at[j, g], dst_ref=rx_own.at[q], send_sem=xd_send.at[j, g], recv_sem=xd_recv.at[q],
            device_id=at_x(j), device_id_type=MESH,
        )

    def pr_copy(q):
        return pltpu.make_async_remote_copy(
            src_ref=rx_own.at[q], dst_ref=rx_par.at[q], send_sem=pr_send.at[q], recv_sem=pr_recv.at[q],
            device_id=partner, device_id_type=MESH,
        )

    def emit(g):
        for j in [*range(1, NX), 0]:
            packed = nn(squeeze, gs[j, g]).astype(BF16)
            if j:
                gd[j, g] = packed
                xd_copy(j, g, x * 2 + g).start()
            else:
                rx_own[x * 2 + g] = packed
                pr_copy(x * 2 + g).start()

    select(0)

    def z_step(s):
        for h in range(2):
            for way in range(2):
                z_copy(way, s, h).wait_recv()
                z_copy(way, s + 1, h).start()
        select(s)
        select(NZ - s)

    @pl.loop(1, grp // 2)
    def _(s):
        z_step(s)

    def late(s):
        for h in range(2):
            for way in range(2):
                if way == 0 or s < grp:
                    z_copy(way, s, h).wait_recv()
                if s + 1 < grp or (way == 0 and s + 1 == grp):
                    z_copy(way, s + 1, h).start()

    def arrive(g):
        for j in range(1, NX):
            q = ((x + NX - j) % NX) * 2 + g
            xd_copy(j, g, q).wait_recv()
            pr_copy(q).start()

    def arrive_partner(g):
        for j in range(NX):
            pr_copy(j * 2 + g).wait_recv()

    half = NY // 2

    def part(g, q, p):
        n, ch = (q // 2) * 2 + g, q % 2
        return nn(rx_own[n][:, :feats], w_own[p, ch]) + nn(rx_par[n][:, :feats], w_par[p, ch])

    def rs_copy(g, way, d, p):
        return pltpu.make_async_remote_copy(
            src_ref=rs_out.at[g, way, d - 1, p], dst_ref=rs_in.at[g, way, d - 1, p],
            send_sem=rs_send.at[g, way, d - 1, p], recv_sem=rs_recv.at[g, way, d - 1, p],
            device_id=at_y(1 if way == 0 else -1), device_id_type=MESH,
        )

    def rs_step(g, way, d, p):
        q = (y + d) % NY if way == 0 else (y + NY - d) % NY
        value = part(g, q, p)
        if d + 1 < half or (d + 1 == half and p == way):
            rs_copy(g, way, d + 1, p).wait_recv()
            value = value + rs_in[g, way, d, p].astype(F32)
        rs_out[g, way, d - 1, p] = value.astype(BF16)
        rs_copy(g, way, d, p).start()

    def rs_pair(g, d, late_half):
        for way in range(2):
            rs_step(g, way, d, way if late_half else 1 - way)

    def rs_first(g):
        rs_pair(g, half, True)
        rs_pair(g, half - 1, False)

    def rs_last(g):
        sums = []
        for p in range(2):
            value = part(g, y, p)
            for way in range(2):
                rs_copy(g, way, 1, p).wait_recv()
                value = value + rs_in[g, way, 0, p].astype(F32)
            sums.append(value)
        hidden = (sums[0] / (1.0 + jnp.exp(-sums[0])) * sums[1]).astype(BF16)
        for p in range(2):
            h_own[g, y, p] = hidden[:, p * hc : (p + 1) * hc]

    def hy_copy(g, way, d, p, q):
        return pltpu.make_async_remote_copy(
            src_ref=h_own.at[g, q, p], dst_ref=h_own.at[g, q, p],
            send_sem=hy_send.at[g, way, d - 1, p], recv_sem=hy_recv.at[g, way, d - 1, p],
            device_id=at_y(1 if way == 0 else -1), device_id_type=MESH,
        )

    def hp_copy(g, q):
        return pltpu.make_async_remote_copy(
            src_ref=h_own.at[g, q], dst_ref=h_par.at[g, q], send_sem=hp_send.at[g, q],
            recv_sem=hp_recv.at[g, q], device_id=partner, device_id_type=MESH,
        )

    def from_y(way, d):
        return (y + NY - d) % NY if way == 0 else (y + d) % NY

    def xr_copy(g, n, i):
        return pltpu.make_async_remote_copy(
            src_ref=o_buf.at[g, n], dst_ref=rb.at[(NX - i) % NX, g], send_sem=xr_send.at[i, g],
            recv_sem=xr_recv.at[(NX - i) % NX, g], device_id=at_x(i), device_id_type=MESH,
        )

    def down(g, step):
        turn = 1 - 2 * (y % 2)
        n = (y // 2 + NX + (0, -turn, turn, 2)[step]) % NX
        acc = None
        for ch in range(2):
            q = n * 2 + ch
            hp_copy(g, q).wait_recv()
            own = jnp.concatenate([h_own[g, q, 0], h_own[g, q, 1]], axis=1)
            par = jnp.concatenate([h_par[g, q, 0], h_par[g, q, 1]], axis=1)
            cols = slice(ch * 2 * hc, (ch + 1) * 2 * hc)
            term = nt(own, wd_own[:, cols]) + nt(par, wd_par[:, cols])
            acc = term if acc is None else acc + term
        o_buf[g, n] = acc.astype(BF16)
        i = (n + NX - x) % NX

        @pl.when(i != 0)
        def _():
            xr_copy(g, n, i).start()

        @pl.when(i == 0)
        def _():
            rb[0, g] = acc.astype(BF16)

    def ag_first(g):
        for p in range(2):
            for way in range(2):
                hy_copy(g, way, 1, p if way == 0 else 1 - p, y).start()
        hp_copy(g, y).start()

    def ag_step(g, d):
        for p in range(2):
            for way in range(2):
                part_no = p if way == 0 else 1 - p
                if d == half and part_no != way:
                    continue
                q = from_y(way, d)
                hy_copy(g, way, d, part_no, q).wait_recv()
                if d + 1 < half or (d + 1 == half and part_no == way):
                    hy_copy(g, way, d + 1, part_no, q).start()
        if d < half:
            for way in range(2):
                hp_copy(g, from_y(way, d)).start()
        else:
            hp_copy(g, from_y(0, d)).start()

    late(grp // 2)
    select(grp // 2)
    emit(0)
    select(NZ - grp // 2)
    late(grp // 2 + 1)
    select(grp // 2 + 1)
    select(NZ - grp // 2 - 1)
    arrive(0)
    late(grp // 2 + 2)
    for copy in w_local:
        copy.wait()
    for copy in w_remote:
        copy.wait_recv()
    arrive_partner(0)
    rs_first(0)
    select(grp - 2)
    select(grp + 2)
    late(grp - 1)
    rs_pair(0, half - 1, True)
    select(grp - 1)
    select(grp + 1)
    rs_pair(0, half - 2, False)
    late(grp)
    select(grp)
    emit(1)
    rs_pair(0, half - 2, True)
    rs_pair(0, half - 3, False)
    arrive(1)
    rs_pair(0, half - 3, True)
    arrive_partner(1)
    rs_first(1)
    rs_last(0)
    rs_pair(1, half - 1, True)
    rs_pair(1, half - 2, False)
    rs_pair(1, half - 2, True)
    rs_pair(1, half - 3, False)
    rs_pair(1, half - 3, True)
    rs_last(1)
    ag_first(1)
    ag_step(1, 1)
    ag_step(1, 2)
    ag_first(0)
    down(1, 0)
    ag_step(1, 3)
    down(1, 1)
    ag_step(1, 4)
    down(1, 2)
    down(1, 3)

    def returned(g):
        for j in range(1, NX):
            xr_copy(g, 0, NX - j).wait_recv()

    iota_row = lax.broadcasted_iota(jnp.int32, (rows, toks), 0).astype(F32)
    zh = feats // 2

    def partial(r):
        g, pos = place(r)
        info = cl[r]
        base = (pos * CAP).astype(F32)
        acc = None
        for j in range(NX):
            code = info[j : j + 1]
            target = jnp.where(code >= 0.0, code + base, -1.0)
            mix = jnp.where(iota_row == target, info[NX + j : NX + j + 1], 0.0).astype(BF16)
            term = tn(rb[j, g], mix)
            acc = term if acc is None else acc + term
        return acc

    def zr_copy(way, d, h):
        return pltpu.make_async_remote_copy(
            src_ref=z_out.at[way, d - 1, h], dst_ref=z_in.at[way, d - 1, h],
            send_sem=zr_send.at[way, d - 1, h], recv_sem=zr_recv.at[way, d - 1, h],
            device_id=at_z(1 if way == 0 else -1), device_id_type=MESH,
        )

    def zr_step(d, takes):
        values = [(way, partial(jnp.asarray(NZ - d if way == 0 else d, jnp.int32))) for way in takes]
        for h in range(2):
            for way, value in values:
                piece = value[h * zh : (h + 1) * zh]
                if takes[way]:
                    zr_copy(way, d + 1, h).wait_recv()
                    piece = piece + z_in[way, d, h].astype(F32)
                z_out[way, d - 1, h] = piece.astype(BF16)
                zr_copy(way, d, h).start()

    ag_step(0, 1)
    returned(1)
    zr_step(grp, {0: False})
    ag_step(0, 2)
    down(0, 0)
    zr_step(grp - 1, {0: True, 1: False})
    ag_step(0, 3)
    down(0, 1)
    zr_step(grp - 2, {0: True, 1: True})
    ag_step(0, 4)
    down(0, 2)
    down(0, 3)
    zr_step(grp - 3, {0: True, 1: True})
    returned(0)

    @pl.loop(0, grp - 4)
    def _(t):
        zr_step(grp - 4 - t, {0: True, 1: True})

    total = partial(jnp.asarray(0, jnp.int32))
    scale = jnp.sum(levels, axis=0, keepdims=True)
    for h in range(2):
        piece = total[h * zh : (h + 1) * zh]
        for way in range(2):
            zr_copy(way, 1, h).wait_recv()
            piece = piece + z_in[way, 0, h].astype(F32)
        out_ref[h * zh : (h + 1) * zh, :] = (piece / scale).astype(BF16)

    for copy in w_remote:
        copy.wait_send()
    for way in range(2):
        for h in range(2):

            @pl.loop(1, grp + 1 - way)
            def _(s, way=way, h=h):
                z_copy(way, s, h).wait_send()
                zr_copy(way, s, h).wait_send()

    for g in range(2):
        for j in range(1, NX):
            xd_copy(j, g, 0).wait_send()
            xr_copy(g, 0, j).wait_send()
        for q in range(NY):
            hp_copy(g, q).wait_send()
        for way in range(2):
            for d in range(1, half + 1):
                for p in range(2):
                    if d < half or p == way:
                        rs_copy(g, way, d, p).wait_send()
                        hy_copy(g, way, d, p, 0).wait_send()
    for q in range(NY):
        pr_copy(q).wait_send()


def on_device(tokens, routes, gate_levels, w_gate, w_up, w_down):
    toks, feats = tokens.shape
    ff = w_gate.shape[2]
    low = 128
    grp = NZ // 2
    rows = grp * CAP
    half = NY // 2
    dma = pltpu.SemaphoreType.DMA
    out = pl.pallas_call(
        kernel,
        out_shape=jax.ShapeDtypeStruct((feats, toks), BF16),
        in_specs=[pl.BlockSpec(memory_space=pl.ANY)]
        + [pl.BlockSpec(memory_space=pltpu.VMEM)] * 2
        + [pl.BlockSpec(memory_space=pl.ANY)] * 3,
        out_specs=pl.BlockSpec(memory_space=pltpu.VMEM),
        scratch_shapes=[
            pltpu.VMEM((NZ, 2, low, toks), BF16),
            pltpu.VMEM((NZ, 2 * NX, toks), F32),
            pltpu.VMEM((NX, 2, grp * SLOT, 2 * low), BF16),
            pltpu.VMEM((NX, 2, rows, 2 * low), BF16),
            pltpu.VMEM((NY, rows, 2 * low), BF16),
            pltpu.VMEM((NY, rows, 2 * low), BF16),
            pltpu.VMEM((2, 2, feats, ff // 4), BF16),
            pltpu.VMEM((2, 2, feats, ff // 4), BF16),
            pltpu.VMEM((feats, ff // 2), BF16),
            pltpu.VMEM((feats, ff // 2), BF16),
            pltpu.VMEM((2, 2, half, 2, rows, ff // 4), BF16),
            pltpu.VMEM((2, 2, half, 2, rows, ff // 4), BF16),
            pltpu.VMEM((2, NY, 2, rows, ff // 8), BF16),
            pltpu.VMEM((2, NY, 2, rows, ff // 8), BF16),
            pltpu.VMEM((2, NX, rows, feats), BF16),
            pltpu.VMEM((NX, 2, rows, feats), BF16),
            pltpu.VMEM((2, grp, 2, feats // 2, toks), BF16),
            pltpu.VMEM((2, grp, 2, feats // 2, toks), BF16),
            dma((2,)), dma((6,)), dma((4,)), dma((4,)),
            dma((2, grp + 1, 2)), dma((2, grp + 1, 2)),
            dma((NX, 2)), dma((NY,)),
            dma((NY,)), dma((NY,)),
            dma((2, 2, half, 2)), dma((2, 2, half, 2)),
            dma((2, 2, half, 2)), dma((2, 2, half, 2)),
            dma((2, NY)), dma((2, NY)),
            dma((NX, 2)), dma((NX, 2)),
            dma((2, grp, 2)), dma((2, grp, 2)),
        ],
        compiler_params=pltpu.CompilerParams(
            collective_id=0, has_side_effects=True, vmem_limit_bytes=60 * 1024 * 1024
        ),
    )(
        tokens.T, routes.T, gate_levels.T,
        w_gate.reshape(feats, ff), w_up.reshape(feats, ff), w_down.reshape(ff, feats).T,
    )
    return out.T


def solution(mesh):
    in_specs = (
        P("ep", "tp"),
        P("ep", None),
        P("ep", None),
        P("ep", "tp", None),
        P("ep", "tp", None),
        P("ep", None, "tp"),
    )
    out_specs = P("ep", "tp")
    return jax.shard_map(
        on_device, mesh=mesh, in_specs=in_specs, out_specs=out_specs, check_vma=False
    )
```
